32 devices in a mesh: rep: 2 (over y), seq: 8 (over z, x), head: 2 (over core).
Axes of the slice: x: 2, y: 2, z: 4, core: 2. Of those that a mesh axis runs over, the one named last changes fastest.
Arguments:
- prompt_query: bfloat16 [2048, 1792], P(('rep', 'seq', 'head')), parts along dimension 0, may hold values from -12 to 12
- prompt_key: bfloat16 [2048, 256], P(('rep', 'seq', 'head')), parts along dimension 0, may hold values from -12 to 12
- prompt_value: bfloat16 [2048, 256], P(('rep', 'seq', 'head')), parts along dimension 0, may hold values from -24 to 24
- prompt_length: int32 [2], P('rep'), parts along dimension 0, may hold values from 512 to 1024
- span_order: int32 [32], P('rep'), parts along dimension 0, may hold values from 0 to 15, each once
- new_query: bfloat16 [32, 1792], P('rep', 'head'), parts along dimension 0, may hold values from -12 to 12
- new_key: bfloat16 [32, 256], P('rep', 'head'), parts along dimension 0, may hold values from -12 to 12
- new_value: bfloat16 [32, 256], P('rep', 'head'), parts along dimension 0, may hold values from -24 to 24
- cache_key: bfloat16 [32, 2, 2048, 128], P('rep', 'head', 'seq'), parts along dimension 0, may hold values from -12 to 12
- cache_value: bfloat16 [32, 2, 2048, 128], P('rep', 'head', 'seq'), parts along dimension 0, may hold values from -24 to 24
- cache_length: int32 [32], P('rep'), parts along dimension 0, may hold values from 1280 to 2048
Outputs:
- prompt_attended: bfloat16 [2048, 1792], P(('rep', 'seq', 'head')), parts along dimension 0
- decode_attended: bfloat16 [32, 1792], P('rep', 'head'), parts along dimension 0
The draws below stay inside these ranges and needn't reach their ends.
There are 2 independent parts, one for each index of `rep`. The reference program is written for one: setup_inputs(seed, part) draws one part's arguments, and reference() takes and returns one part's arrays. A program takes and returns all parts, laid end to end along the dimension named above; each array names one. Nothing has to cross between parts.
Inputs may be any that keep to these rules, and one draw needn't show every extreme that they name: `span_order`: each of the 16 spans stands once.
All inputs are finite; a program needn't handle non-finite values.
Results may differ from the reference program's by a relative error of at most 0.0045.
Values may be sent and summed in bfloat16 or wider, within the bound.
A program may use at most 128 MiB of HBM per device.

```python
import math
import jax
import jax.numpy as jnp
from jax import lax

HD = 128
QH = 14
KVH = 2
SPAN = 64
SESS = 16
CTX_DEV = 256
NCHUNK = 16
PROMPT = 1024
CTX = 2048


def prompt_fields(key):
    query_key = jax.random.fold_in(key, 31)
    keys_key = jax.random.fold_in(key, 32)
    broad_key = jax.random.fold_in(key, 34)
    row_ids = jnp.arange(PROMPT, dtype=jnp.int32)
    queries = 1.2 * jnp.clip(jax.random.normal(query_key, (PROMPT, QH * HD), jnp.float32), -6.0, 6.0)
    broad = jax.random.uniform(broad_key, (PROMPT, QH * HD), jnp.float32, -6.0, 6.0)
    broad_rows = row_ids % 64 == 5
    queries = jnp.where(broad_rows[:, None], broad, queries)
    keys_drawn = 1.2 * jnp.clip(jax.random.normal(keys_key, (PROMPT, KVH * HD), jnp.float32), -6.0, 6.0)
    return (queries, keys_drawn)


def decode_fields(key):
    query_key = jax.random.fold_in(key, 41)
    keys_key = jax.random.fold_in(key, 42)
    broad_key = jax.random.fold_in(key, 44)
    session_ids = jnp.arange(SESS, dtype=jnp.int32)
    queries = 1.2 * jnp.clip(jax.random.normal(query_key, (SESS, QH * HD), jnp.float32), -6.0, 6.0)
    broad = jax.random.uniform(broad_key, (SESS, QH * HD), jnp.float32, -6.0, 6.0)
    broad_rows = session_ids % 4 == 1
    queries = jnp.where(broad_rows[:, None], broad, queries)
    keys_drawn = 1.2 * jnp.clip(jax.random.normal(keys_key, (SESS, KVH, CTX, HD), jnp.float32), -6.0, 6.0)
    far_slot = CTX // 2 + CTX_DEV // 2
    planted_scale = 5.0 / (1.44 * math.sqrt(HD))
    leading = queries.reshape(SESS, KVH, QH // KVH, HD)[:, :, 0, :]
    keys_drawn = keys_drawn.at[:, :, far_slot, :].set(planted_scale * leading)
    return (queries, keys_drawn)


def draw_prompt_query(key, part):
    return prompt_fields(key)[0].astype(jnp.bfloat16)


def draw_prompt_key(key, part):
    return prompt_fields(key)[1].astype(jnp.bfloat16)


def draw_new_query(key, part):
    return decode_fields(key)[0].astype(jnp.bfloat16)


def draw_cache_key(key, part):
    return decode_fields(key)[1].astype(jnp.bfloat16)


def plant(values, key, low, top_value):
    longest = values.shape.index(max(values.shape))
    spots = []
    for shift in (0, 1):
        where = [jax.random.randint(jax.random.fold_in(key, axis), (), 0, length) for axis, length in enumerate(values.shape)]
        where[longest] = (where[longest] + shift) % values.shape[longest]
        spots.append(tuple(where))
    return values.at[spots[0]].set(low).at[spots[1]].set(top_value)


def level_of(key, shape, split, least, high):
    factor_of = 1.0
    for position, shards_of in split:
        draws = jax.random.uniform(jax.random.fold_in(jax.random.fold_in(key, 6), position), (shards_of,), jnp.float32, least / len(split), high / len(split))
        factor_of = factor_of * jnp.repeat(jnp.exp(draws), shape[position] // shards_of).reshape((-1,) + (1,) * (len(shape) - 1 - position))
    return factor_of


def scatter_about(key, shape, width, most, shards=(), kind=jnp.bfloat16):
    values = jax.random.normal(key, shape, jnp.float32) * width
    if len(shards) > 0:
        values = level_of(key, shape, shards, -0.22, 0.18) * values
    return jnp.clip(values, min=-most, max=most).astype(kind)


def setup_inputs(seed: int = 0, part: int = 0) -> dict:
    keys = jax.random.split(jax.random.key(seed), 12)
    part_splits = jax.random.split(jax.random.fold_in(keys[11], part), 12)
    return {
        "prompt_query": draw_prompt_query(jax.random.fold_in(jax.random.fold_in(keys[11], part), 71), part),
        "prompt_key": draw_prompt_key(jax.random.fold_in(jax.random.fold_in(keys[11], part), 71), part),
        "prompt_value": scatter_about(part_splits[2], (PROMPT, KVH * HD), 4.0, 24.0, ((0, 16),)),
        "prompt_length": jax.random.randint(part_splits[3], (1,), PROMPT // 2, PROMPT + 1).astype(jnp.int32),
        "span_order": jax.random.permutation(part_splits[4], NCHUNK).astype(jnp.int32),
        "new_query": draw_new_query(jax.random.fold_in(jax.random.fold_in(keys[11], part), 71), part),
        "new_key": scatter_about(part_splits[6], (SESS, KVH * HD), 2.0, 12.0, ((1, 2),)),
        "new_value": scatter_about(part_splits[7], (SESS, KVH * HD), 4.0, 24.0, ((1, 2),)),
        "cache_key": draw_cache_key(jax.random.fold_in(jax.random.fold_in(keys[11], part), 71), part),
        "cache_value": scatter_about(part_splits[9], (SESS, KVH, CTX, HD), 4.0, 24.0, ((1, 2), (2, 8))),
        "cache_length": plant(jax.random.randint(part_splits[10], (SESS,), CTX // 2 + CTX_DEV, CTX + 1), jax.random.fold_in(part_splits[10], 1), CTX // 2 + CTX_DEV, CTX).astype(jnp.int32),
    }


def reference(prompt_query, prompt_key, prompt_value, prompt_length, span_order, new_query, new_key, new_value, cache_key, cache_value, cache_length):
    head_group = QH // KVH
    score_scale = 1.0 / math.sqrt(HD)
    row_ids = jnp.arange(PROMPT, dtype=jnp.int32)
    positions = (span_order[row_ids // SPAN] * SPAN + row_ids % SPAN).astype(jnp.int32)
    length_limit = prompt_length[0]
    key_table = prompt_key.astype(jnp.float32).reshape(PROMPT, KVH, HD)
    value_table = prompt_value.astype(jnp.float32).reshape(PROMPT, KVH, HD)
    key_live = positions < length_limit
    block_rows = math.gcd(PROMPT, 256)

    def one_block(block_index):
        start_row = (block_index * block_rows).astype(jnp.int32)
        queries = lax.dynamic_slice_in_dim(prompt_query, start_row, block_rows, 0).astype(jnp.float32)
        queries = queries.reshape(block_rows, KVH, head_group, HD)
        query_pos = lax.dynamic_slice_in_dim(positions, start_row, block_rows, 0)
        scores = jnp.einsum('rkgd,nkd->kgrn', queries, key_table) * score_scale
        allowed = (positions[None, :] <= query_pos[:, None]) & key_live[None, :]
        scores = jnp.where(allowed, scores, -1e+30)
        row_max = lax.optimization_barrier(jnp.max(scores, axis=-1, keepdims=True))
        weights = jnp.where(allowed, jnp.exp(scores - row_max), 0.0)
        row_total = lax.optimization_barrier(jnp.sum(weights, axis=-1))
        rounded = lax.optimization_barrier(weights.astype(jnp.bfloat16)).astype(jnp.float32)
        weighted = jnp.einsum('kgrn,nkd->rkgd', rounded, value_table)
        result = weighted / jnp.transpose(row_total, (2, 0, 1))[..., None]
        result = jnp.where((query_pos < length_limit)[:, None, None, None], result, 0.0)
        return result.reshape(block_rows, QH * HD).astype(jnp.bfloat16)
    prompt_attended = lax.map(one_block, jnp.arange(PROMPT // block_rows, dtype=jnp.int32)).reshape(PROMPT, QH * HD)
    cache_pos = jnp.arange(CTX, dtype=jnp.int32)

    def one_session(session):
        queries = new_query[session].astype(jnp.float32).reshape(KVH, head_group, HD)
        keys_here = cache_key[session].astype(jnp.float32)
        values_here = cache_value[session].astype(jnp.float32)
        fresh_key = new_key[session].astype(jnp.float32).reshape(KVH, HD)
        fresh_value = new_value[session].astype(jnp.float32).reshape(KVH, HD)
        valid = cache_pos < cache_length[session]
        scores = jnp.einsum('kgd,ktd->kgt', queries, keys_here) * score_scale
        scores = jnp.where(valid[None, None, :], scores, -1e+30)
        own_score = jnp.einsum('kgd,kd->kg', queries, fresh_key) * score_scale
        row_max = jnp.maximum(lax.optimization_barrier(jnp.max(scores, axis=-1)), own_score)
        weights = jnp.where(valid[None, None, :], jnp.exp(scores - row_max[..., None]), 0.0)
        own_weight = jnp.exp(own_score - row_max)
        row_total = lax.optimization_barrier(jnp.sum(weights, axis=-1)) + own_weight
        rounded = lax.optimization_barrier(weights.astype(jnp.bfloat16)).astype(jnp.float32)
        own_rounded = lax.optimization_barrier(own_weight.astype(jnp.bfloat16)).astype(jnp.float32)
        weighted = jnp.einsum('kgt,ktd->kgd', rounded, values_here) + own_rounded[..., None] * fresh_value[:, None, :]
        return (weighted / row_total[..., None]).reshape(QH * HD).astype(jnp.bfloat16)
    decode_attended = lax.map(one_session, jnp.arange(SESS, dtype=jnp.int32))
    return (prompt_attended, decode_attended)
```

```python
import functools
import math

import jax
import jax.numpy as jnp
from jax import lax
from jax.experimental import pallas as pl
from jax.experimental.pallas import tpu as pltpu
from jax.sharding import PartitionSpec as P

HD = 128
QH = 14
KVH = 2


def lookup(span_table, row_ids, span_rows):
    chosen = (
        row_ids[:, None] // span_rows == jnp.arange(span_table.shape[0], dtype=jnp.int32)[None, :]
    )
    picked = jnp.sum(jnp.where(chosen, span_table[None, :], 0), axis=1)
    return picked * span_rows + row_ids % span_rows


def block_size(key_count, span_rows):
    units = key_count // span_rows
    most = max(1, 512 // span_rows)
    best = 1
    for count in range(1, min(units, most) + 1):
        if units % count == 0:
            best = count
    return best * span_rows


def start_state(query_rows, kv_heads, head_group):
    row_max = jnp.full((kv_heads, head_group, query_rows), -1e30, jnp.float32)
    row_total = jnp.zeros((kv_heads, head_group, query_rows), jnp.float32)
    weighted = jnp.zeros((kv_heads, head_group, query_rows, HD), jnp.float32)
    return (row_max, row_total, weighted)


def attend_rows(running, shard_piece, queries, query_pos, span_table, span_rows, length_limit):
    keys_piece, values_piece = shard_piece
    key_count = keys_piece.shape[0]
    kv_heads = queries.shape[1]
    block_rows = block_size(key_count, span_rows)
    score_scale = 1.0 / math.sqrt(HD)

    def advance(carried, block_index):
        first_row = block_index * block_rows
        key_block = lax.dynamic_slice_in_dim(keys_piece, first_row, block_rows, 0).reshape(
            block_rows, kv_heads, HD
        )
        value_block = lax.dynamic_slice_in_dim(values_piece, first_row, block_rows, 0).reshape(
            block_rows, kv_heads, HD
        )
        key_pos = lookup(span_table, first_row + jnp.arange(block_rows, dtype=jnp.int32), span_rows)
        allowed = (key_pos[None, :] <= query_pos[:, None]) & (key_pos[None, :] < length_limit)

        def compute(state_in):
            row_max, row_total, weighted = state_in
            scores = (
                jnp.einsum("rkgd,nkd->kgrn", queries, key_block, preferred_element_type=jnp.float32)
                * score_scale
            )
            scores = jnp.where(allowed, scores, -1e30)
            new_max = jnp.maximum(row_max, jnp.max(scores, axis=-1))
            weights = jnp.where(allowed, jnp.exp(scores - new_max[..., None]), 0.0)
            factor = jnp.exp(row_max - new_max)
            row_total = row_total * factor + jnp.sum(weights, axis=-1)
            weighted = weighted * factor[..., None] + jnp.einsum(
                "kgrn,nkd->kgrd",
                weights.astype(jnp.bfloat16),
                value_block,
                preferred_element_type=jnp.float32,
            )
            return (new_max, row_total, weighted)

        return (lax.cond(jnp.any(allowed), compute, lambda state_in: state_in, carried), None)

    running, _ = lax.scan(advance, running, jnp.arange(key_count // block_rows, dtype=jnp.int32))
    return running


def finish(running, query_pos, length_limit):
    row_max, row_total, weighted = running
    result = weighted / row_total[..., None]
    result = jnp.transpose(result, (2, 0, 1, 3))
    result = jnp.where((query_pos < length_limit)[:, None, None, None], result, 0.0)
    return result.reshape(result.shape[0], -1).astype(jnp.bfloat16)


def composed(
    prompt_query,
    prompt_key,
    prompt_value,
    prompt_length,
    span_order,
    new_query,
    new_key,
    new_value,
    cache_key,
    cache_value,
    cache_length,
):
    head_group = QH // KVH
    score_scale = 1.0 / math.sqrt(HD)
    length_limit = prompt_length[0]
    span_rows = prompt_query.shape[0]
    kv_heads = prompt_key.shape[1] // HD
    first_row = (lax.axis_index("seq") * lax.axis_size("head") + lax.axis_index("head")) * span_rows
    query_pos = lookup(span_order, first_row + jnp.arange(span_rows, dtype=jnp.int32), span_rows)
    queries = prompt_query.reshape(span_rows, kv_heads, head_group, HD)
    running = attend_rows(
        start_state(span_rows, kv_heads, head_group),
        (
            lax.all_gather(prompt_key, ("seq", "head"), axis=0, tiled=True),
            lax.all_gather(prompt_value, ("seq", "head"), axis=0, tiled=True),
        ),
        queries,
        query_pos,
        span_order,
        span_rows,
        length_limit,
    )
    prompt_attended = finish(running, query_pos, length_limit)
    sessions = new_query.shape[0]
    local_heads = cache_key.shape[1]
    local_ctx = cache_key.shape[2]
    dec_queries = new_query.reshape(sessions, local_heads, head_group, HD)
    cache_pos = lax.axis_index("seq") * local_ctx + jnp.arange(local_ctx, dtype=jnp.int32)
    valid = (cache_pos[None, :] < cache_length[:, None])[:, None, None, :]
    scores = (
        jnp.einsum("skgd,sktd->skgt", dec_queries, cache_key, preferred_element_type=jnp.float32)
        * score_scale
    )
    scores = jnp.where(valid, scores, -1e30)
    row_max = jnp.max(scores, axis=-1)
    weights = jnp.where(valid, jnp.exp(scores - row_max[..., None]), 0.0)
    row_total = jnp.sum(weights, axis=-1)
    weighted = jnp.einsum(
        "skgt,sktd->skgd",
        weights.astype(jnp.bfloat16),
        cache_value,
        preferred_element_type=jnp.float32,
    )
    global_max = lax.pmax(row_max, "seq")
    factor = jnp.exp(row_max - global_max)
    row_total, weighted = lax.psum((row_total * factor, weighted * factor[..., None]), "seq")
    row_max = global_max
    own_score = (
        jnp.einsum(
            "skgd,skd->skg",
            dec_queries,
            new_key.reshape(sessions, local_heads, HD),
            preferred_element_type=jnp.float32,
        )
        * score_scale
    )
    final_max = jnp.maximum(row_max, own_score)
    old_factor = jnp.exp(row_max - final_max)
    own_weight = jnp.exp(own_score - final_max)
    row_total = row_total * old_factor + own_weight
    own_rounded = lax.optimization_barrier(own_weight.astype(jnp.bfloat16)).astype(jnp.float32)
    fresh_value = new_value.reshape(sessions, local_heads, 1, HD).astype(jnp.float32)
    weighted = weighted * old_factor[..., None] + own_rounded[..., None] * fresh_value
    decode_attended = (weighted / row_total[..., None]).reshape(sessions, -1).astype(jnp.bfloat16)
    return (prompt_attended, decode_attended)


MESH = pl.DeviceIdType.MESH
LOW = -1e30
FAR = 1 << 30


def pick(index, table):
    out = jnp.int32(table[0])
    for i in range(1, len(table)):
        out = jnp.where(index == i, jnp.int32(table[i]), out)
    return out


def fused_kernel(
    outer, inner, cores,
    pq_hbm, pk_hbm, pv_hbm, length_ref, order_ref, nq_ref, nk_ref, nv_ref, ck_hbm, cv_hbm, clen_ref,
    out_ref, dec_ref,
    pq, kbuf, vbuf, ck, cv, qrows, part_out, part_in, done, flat,
    in_sem, kv_send, kv_recv, part_send, part_recv, done_send, done_recv,
):
    group = QH // KVH
    span = kbuf.shape[1] // (inner * cores)
    n_seq = outer * inner
    seq = lax.axis_index("seq")
    core = lax.axis_index("head")
    a = seq // inner
    b = seq % inner
    log2_scale = math.log2(math.e) / math.sqrt(HD)

    def rows_of(b_, c_):
        return pl.ds(pl.multiple_of((b_ * cores + c_) * span, span), span)

    def block_id(a_, b_, c_):
        return (a_ * inner + b_) * cores + c_

    local = [
        pltpu.make_async_copy(pk_hbm, kbuf.at[a, rows_of(b, core)], in_sem.at[0]),
        pltpu.make_async_copy(pv_hbm, vbuf.at[a, rows_of(b, core)], in_sem.at[1]),
        pltpu.make_async_copy(ck_hbm, ck, in_sem.at[2]),
        pltpu.make_async_copy(cv_hbm, cv, in_sem.at[3]),
        pltpu.make_async_copy(pq_hbm, pq, in_sem.at[4]),
    ]
    for copy in local:
        copy.start()

    barrier = pltpu.get_barrier_semaphore()
    for d in range(1, n_seq):
        pl.semaphore_signal(
            barrier, inc=1, device_id={"seq": (seq + d) % n_seq}, device_id_type=MESH
        )
    for d in range(1, cores):
        pl.semaphore_signal(
            barrier, inc=1, device_id={"head": (core + d) % cores}, device_id_type=MESH
        )
    local[0].wait()
    local[1].wait()
    pl.semaphore_wait(barrier, n_seq - 1 + cores - 1)

    sends = []

    def send(a_, b_, c_, target):
        block = block_id(a_, b_, c_)
        for which, buf in ((0, kbuf), (1, vbuf)):
            ref = buf.at[a_, rows_of(b_, c_)]
            copy = pltpu.make_async_remote_copy(
                src_ref=ref,
                dst_ref=ref,
                send_sem=kv_send.at[which, len(sends) // 2],
                recv_sem=kv_recv.at[which, block],
                device_id=target,
                device_id_type=MESH,
            )
            copy.start()
            sends.append(copy)

    def await_block(a_, b_, c_):
        block = block_id(a_, b_, c_)
        for which, buf in ((0, kbuf), (1, vbuf)):
            ref = buf.at[a_, rows_of(b_, c_)]
            pltpu.make_async_remote_copy(
                src_ref=ref,
                dst_ref=ref,
                send_sem=kv_send.at[which, 0],
                recv_sem=kv_recv.at[which, block],
                device_id={"seq": seq},
                device_id_type=MESH,
            ).wait_recv()

    def to_inner(a_, b_, c_):
        for d in range(1, inner):
            send(a_, b_, c_, {"seq": a * inner + (b + d) % inner})

    def to_core(a_, b_, c_):
        for d in range(1, cores):
            send(a_, b_, c_, {"head": (core + d) % cores})

    nearest = [sorted(range(outer), key=lambda p, i=i: (abs(p - i), p)) for i in range(outer)]
    planes = [pick(a, [nearest[i][k] for i in range(outer)]) for k in range(outer)]

    to_inner(a, b, core)
    for k in range(1, outer):
        send(a, b, core, {"seq": planes[k] * inner + b})
    to_core(a, b, core)

    sessions, ctx = ck.shape[0], ck.shape[2]
    per = sessions // n_seq
    for h in range(8):
        if h < group:
            qrows[pl.ds(h * sessions, sessions), :] = nq_ref[:, h * HD : (h + 1) * HD].astype(
                jnp.float32
            )
        else:
            qrows[pl.ds(h * sessions, sessions), :] = jnp.zeros((sessions, HD), jnp.float32)
    local[2].wait()
    local[3].wait()
    cache_pos = seq * ctx + lax.broadcasted_iota(jnp.int32, (8, ctx), 1)
    first = seq == 0
    nk = nk_ref[...].astype(jnp.float32)
    nv = nv_ref[...].astype(jnp.float32)
    inv = 1.0 / math.sqrt(HD)
    for s in range(sessions):
        q32 = qrows[pl.ds(s, 8, stride=sessions), :]
        sc = lax.dot_general(
            q32.astype(jnp.bfloat16), ck[s, 0], (((1,), (1,)), ((), ())),
            preferred_element_type=jnp.float32,
        ) * inv
        own = jnp.sum(q32 * nk[s : s + 1, :], axis=1, keepdims=True) * inv
        own = jnp.where(first, own, LOW)
        valid = cache_pos < clen_ref[s]
        sc = jnp.where(valid, sc, LOW)
        top = jnp.maximum(jnp.max(sc, axis=1, keepdims=True), own)
        w = jnp.where(valid, jnp.exp(sc - top), 0.0)
        own_w = jnp.where(first, jnp.exp(own - top), 0.0)
        tot = jnp.sum(w, axis=1, keepdims=True) + own_w
        o = jnp.dot(w.astype(jnp.bfloat16), cv[s, 0], preferred_element_type=jnp.float32)
        o = o + own_w.astype(jnp.bfloat16).astype(jnp.float32) * nv[s : s + 1, :]
        lane = lax.broadcasted_iota(jnp.int32, (8, HD), 1)
        dst, row = s // per, (s % per) * 8
        part_out[dst, 0, pl.ds(row, 8), :] = o
        part_out[dst, 1, pl.ds(row, 8), :] = jnp.where(lane < HD // 2, top, tot)

    part_copies = []
    for d in range(1, n_seq):
        peer = (seq + d) % n_seq
        copy = pltpu.make_async_remote_copy(
            src_ref=part_out.at[peer],
            dst_ref=part_in.at[n_seq - 1 - d],
            send_sem=part_send.at[d - 1],
            recv_sem=part_recv.at[n_seq - 1 - d],
            device_id={"seq": peer},
            device_id_type=MESH,
        )
        copy.start()
        part_copies.append(copy)

    local[4].wait()
    me_block = block_id(a, b, core)
    limit = length_ref[0]
    rows = group * span
    row_pos = order_ref[me_block] * span + lax.broadcasted_iota(jnp.int32, (rows, 1), 0) % span
    keys = kbuf.shape[1]
    lane = lax.broadcasted_iota(jnp.int32, (1, keys), 1)
    queries = [
        jnp.concatenate(
            [pq[:, (g * group + h) * HD : (g * group + h + 1) * HD] for h in range(group)], axis=0
        )
        for g in range(KVH)
    ]
    state = [None] * KVH

    def attend(a_):
        base = jnp.zeros((1, keys), jnp.int32)
        for j in range(inner * cores):
            base = jnp.where(lane // span == j, order_ref[a_ * inner * cores + j], base)
        key_pos = base * span + lane % span
        key_pos = jnp.where(key_pos < limit, key_pos, FAR)
        allowed = key_pos <= row_pos
        for g in range(KVH):
            kk = kbuf[a_, :, g * HD : (g + 1) * HD]
            vv = vbuf[a_, :, g * HD : (g + 1) * HD]
            sc = lax.dot_general(
                queries[g], kk, (((1,), (1,)), ((), ())), preferred_element_type=jnp.float32
            )
            sc = jnp.where(allowed, sc, LOW)
            best = jnp.max(sc, axis=1, keepdims=True)
            if state[g] is not None:
                best = jnp.maximum(best, state[g][0])
            w = jnp.exp2((sc - best) * log2_scale)
            tot = jnp.sum(w, axis=1, keepdims=True)
            o = jnp.dot(w.astype(jnp.bfloat16), vv, preferred_element_type=jnp.float32)
            if state[g] is not None:
                old, old_tot, old_o = state[g]
                f = jnp.exp2((old - best) * log2_scale)
                tot = tot + old_tot * f
                o = o + old_o * f
            state[g] = (best, tot, o)

    def decode_combine():
        for k in range(n_seq - 1):
            pltpu.make_async_remote_copy(
                src_ref=part_out.at[0],
                dst_ref=part_in.at[k],
                send_sem=part_send.at[0],
                recv_sem=part_recv.at[k],
                device_id={"seq": seq},
                device_id_type=MESH,
            ).wait_recv()
        parts = [part_out[seq]] + [part_in[k] for k in range(n_seq - 1)]
        tops = [p[1][:, 0:1] for p in parts]
        tots = [p[1][:, HD - 1 : HD] for p in parts]
        top = functools.reduce(jnp.maximum, tops)
        fs = [jnp.exp(t - top) for t in tops]
        tot = sum(f * t for f, t in zip(fs, tots))
        o = sum(f * p[0] for f, p in zip(fs, parts))
        done[seq] = (o / tot).astype(jnp.bfloat16)
        copies = []
        for d in range(1, n_seq):
            peer = (seq + d) % n_seq
            copy = pltpu.make_async_remote_copy(
                src_ref=done.at[seq],
                dst_ref=done.at[seq],
                send_sem=done_send.at[d - 1],
                recv_sem=done_recv.at[seq],
                device_id={"seq": peer},
                device_id_type=MESH,
            )
            copy.start()
            copies.append(copy)
        return copies

    done_copies = []
    for k in range(outer):
        if k + 1 < outer:
            await_block(planes[k + 1], b, core)
            to_inner(planes[k + 1], b, core)
            to_core(planes[k + 1], b, core)
        for d in range(1, inner):
            await_block(planes[k], (b + d) % inner, core)
            to_core(planes[k], (b + d) % inner, core)
        if k == outer - 1:
            done_copies = decode_combine()
        for d in range(1, cores):
            for d2 in range(inner):
                await_block(planes[k], (b + d2) % inner, (core + d) % cores)
        attend(planes[k])

    live = row_pos < limit
    for g in range(KVH):
        _, tot, o = state[g]
        res = jnp.where(live, o / tot, 0.0).astype(jnp.bfloat16)
        for h in range(group):
            out_ref[:, (g * group + h) * HD : (g * group + h + 1) * HD] = res[
                h * span : (h + 1) * span
            ]

    for d in range(1, n_seq):
        peer = (seq + d) % n_seq
        pltpu.make_async_remote_copy(
            src_ref=done.at[peer],
            dst_ref=done.at[peer],
            send_sem=done_send.at[0],
            recv_sem=done_recv.at[peer],
            device_id={"seq": seq},
            device_id_type=MESH,
        ).wait_recv()
    flat[...] = done[...].reshape(flat.shape).astype(jnp.float32)
    for h in range(group):
        dec_ref[:, h * HD : (h + 1) * HD] = flat[pl.ds(h, sessions, stride=8), :].astype(
            jnp.bfloat16
        )
    for copy in sends + part_copies + done_copies:
        copy.wait_send()


def fused(outer, inner, cores, *args):
    pq, pk, pv, length, order, nq, nk, nv, ck, cv, clen = args
    span = pq.shape[0]
    sessions = nq.shape[0]
    n_seq = outer * inner
    per = sessions // n_seq
    n_sends = (outer - 1) + outer * (inner - 1) + n_seq * (cores - 1)
    keys = inner * cores * span
    hbm = pl.BlockSpec(memory_space=pl.ANY)
    vmem = pl.BlockSpec(memory_space=pltpu.VMEM)
    smem = pl.BlockSpec(memory_space=pltpu.SMEM)
    dma = pltpu.SemaphoreType.DMA
    return pl.pallas_call(
        functools.partial(fused_kernel, outer, inner, cores),
        name="attention",
        out_shape=(
            jax.ShapeDtypeStruct(pq.shape, jnp.bfloat16),
            jax.ShapeDtypeStruct(nq.shape, jnp.bfloat16),
        ),
        in_specs=[hbm, hbm, hbm, smem, smem, vmem, vmem, vmem, hbm, hbm, smem],
        out_specs=(vmem, vmem),
        scratch_shapes=[
            pltpu.VMEM(pq.shape, jnp.bfloat16),
            pltpu.VMEM((outer, keys, pk.shape[1]), jnp.bfloat16),
            pltpu.VMEM((outer, keys, pv.shape[1]), jnp.bfloat16),
            pltpu.VMEM(ck.shape, jnp.bfloat16),
            pltpu.VMEM(cv.shape, jnp.bfloat16),
            pltpu.VMEM((8 * sessions, HD), jnp.float32),
            pltpu.VMEM((n_seq, 2, per * 8, HD), jnp.float32),
            pltpu.VMEM((n_seq - 1, 2, per * 8, HD), jnp.float32),
            pltpu.VMEM((n_seq, per * 8, HD), jnp.bfloat16),
            pltpu.VMEM((8 * sessions, HD), jnp.float32),
            dma((5,)),
            dma((2, n_sends)),
            dma((2, n_seq * cores)),
            dma((n_seq - 1,)),
            dma((n_seq - 1,)),
            dma((n_seq - 1,)),
            dma((n_seq,)),
        ],
        compiler_params=pltpu.CompilerParams(
            collective_id=0, has_side_effects=True, vmem_limit_bytes=48 * 1024 * 1024
        ),
    )(*args)


def per_device(outer, inner, cores, *args):
    sessions, span = args[5].shape[0], args[0].shape[0]
    if sessions % (outer * inner) or span % 16 or QH // KVH > 8:
        return composed(*args)
    return fused(outer, inner, cores, *args)


def solution(mesh):
    n_seq, cores = mesh.shape["seq"], mesh.shape["head"]
    inner = max(d for d in range(1, math.isqrt(n_seq) + 1) if n_seq % d == 0)
    return jax.shard_map(
        functools.partial(per_device, n_seq // inner, inner, cores),
        mesh=mesh,
        in_specs=(
            P(("rep", "seq", "head"), None),
            P(("rep", "seq", "head"), None),
            P(("rep", "seq", "head"), None),
            P("rep"),
            P("rep"),
            P("rep", "head"),
            P("rep", "head"),
            P("rep", "head"),
            P("rep", "head", "seq", None),
            P("rep", "head", "seq", None),
            P("rep"),
        ),
        out_specs=(P(("rep", "seq", "head"), None), P("rep", "head")),
        check_vma=False,
    )
```

```python
import functools
import math

import jax
import jax.numpy as jnp
from jax import lax
from jax.experimental import pallas as pl
from jax.experimental.pallas import tpu as pltpu
from jax.sharding import PartitionSpec as P

HD = 128
QH = 14
KVH = 2


def lookup(span_table, row_ids, span_rows):
    chosen = (
        row_ids[:, None] // span_rows == jnp.arange(span_table.shape[0], dtype=jnp.int32)[None, :]
    )
    picked = jnp.sum(jnp.where(chosen, span_table[None, :], 0), axis=1)
    return picked * span_rows + row_ids % span_rows


def block_size(key_count, span_rows):
    units = key_count // span_rows
    most = max(1, 512 // span_rows)
    best = 1
    for count in range(1, min(units, most) + 1):
        if units % count == 0:
            best = count
    return best * span_rows


def start_state(query_rows, kv_heads, head_group):
    row_max = jnp.full((kv_heads, head_group, query_rows), -1e30, jnp.float32)
    row_total = jnp.zeros((kv_heads, head_group, query_rows), jnp.float32)
    weighted = jnp.zeros((kv_heads, head_group, query_rows, HD), jnp.float32)
    return (row_max, row_total, weighted)


def attend_rows(running, shard_piece, queries, query_pos, span_table, span_rows, length_limit):
    keys_piece, values_piece = shard_piece
    key_count = keys_piece.shape[0]
    kv_heads = queries.shape[1]
    block_rows = block_size(key_count, span_rows)
    score_scale = 1.0 / math.sqrt(HD)

    def advance(carried, block_index):
        first_row = block_index * block_rows
        key_block = lax.dynamic_slice_in_dim(keys_piece, first_row, block_rows, 0).reshape(
            block_rows, kv_heads, HD
        )
        value_block = lax.dynamic_slice_in_dim(values_piece, first_row, block_rows, 0).reshape(
            block_rows, kv_heads, HD
        )
        key_pos = lookup(span_table, first_row + jnp.arange(block_rows, dtype=jnp.int32), span_rows)
        allowed = (key_pos[None, :] <= query_pos[:, None]) & (key_pos[None, :] < length_limit)

        def compute(state_in):
            row_max, row_total, weighted = state_in
            scores = (
                jnp.einsum("rkgd,nkd->kgrn", queries, key_block, preferred_element_type=jnp.float32)
                * score_scale
            )
            scores = jnp.where(allowed, scores, -1e30)
            new_max = jnp.maximum(row_max, jnp.max(scores, axis=-1))
            weights = jnp.where(allowed, jnp.exp(scores - new_max[..., None]), 0.0)
            factor = jnp.exp(row_max - new_max)
            row_total = row_total * factor + jnp.sum(weights, axis=-1)
            weighted = weighted * factor[..., None] + jnp.einsum(
                "kgrn,nkd->kgrd",
                weights.astype(jnp.bfloat16),
                value_block,
                preferred_element_type=jnp.float32,
            )
            return (new_max, row_total, weighted)

        return (lax.cond(jnp.any(allowed), compute, lambda state_in: state_in, carried), None)

    running, _ = lax.scan(advance, running, jnp.arange(key_count // block_rows, dtype=jnp.int32))
    return running


def finish(running, query_pos, length_limit):
    row_max, row_total, weighted = running
    result = weighted / row_total[..., None]
    result = jnp.transpose(result, (2, 0, 1, 3))
    result = jnp.where((query_pos < length_limit)[:, None, None, None], result, 0.0)
    return result.reshape(result.shape[0], -1).astype(jnp.bfloat16)


def composed(
    prompt_query,
    prompt_key,
    prompt_value,
    prompt_length,
    span_order,
    new_query,
    new_key,
    new_value,
    cache_key,
    cache_value,
    cache_length,
):
    head_group = QH // KVH
    score_scale = 1.0 / math.sqrt(HD)
    length_limit = prompt_length[0]
    span_rows = prompt_query.shape[0]
    kv_heads = prompt_key.shape[1] // HD
    first_row = (lax.axis_index("seq") * lax.axis_size("head") + lax.axis_index("head")) * span_rows
    query_pos = lookup(span_order, first_row + jnp.arange(span_rows, dtype=jnp.int32), span_rows)
    queries = prompt_query.reshape(span_rows, kv_heads, head_group, HD)
    running = attend_rows(
        start_state(span_rows, kv_heads, head_group),
        (
            lax.all_gather(prompt_key, ("seq", "head"), axis=0, tiled=True),
            lax.all_gather(prompt_value, ("seq", "head"), axis=0, tiled=True),
        ),
        queries,
        query_pos,
        span_order,
        span_rows,
        length_limit,
    )
    prompt_attended = finish(running, query_pos, length_limit)
    sessions = new_query.shape[0]
    local_heads = cache_key.shape[1]
    local_ctx = cache_key.shape[2]
    dec_queries = new_query.reshape(sessions, local_heads, head_group, HD)
    cache_pos = lax.axis_index("seq") * local_ctx + jnp.arange(local_ctx, dtype=jnp.int32)
    valid = (cache_pos[None, :] < cache_length[:, None])[:, None, None, :]
    scores = (
        jnp.einsum("skgd,sktd->skgt", dec_queries, cache_key, preferred_element_type=jnp.float32)
        * score_scale
    )
    scores = jnp.where(valid, scores, -1e30)
    row_max = jnp.max(scores, axis=-1)
    weights = jnp.where(valid, jnp.exp(scores - row_max[..., None]), 0.0)
    row_total = jnp.sum(weights, axis=-1)
    weighted = jnp.einsum(
        "skgt,sktd->skgd",
        weights.astype(jnp.bfloat16),
        cache_value,
        preferred_element_type=jnp.float32,
    )
    global_max = lax.pmax(row_max, "seq")
    factor = jnp.exp(row_max - global_max)
    row_total, weighted = lax.psum((row_total * factor, weighted * factor[..., None]), "seq")
    row_max = global_max
    own_score = (
        jnp.einsum(
            "skgd,skd->skg",
            dec_queries,
            new_key.reshape(sessions, local_heads, HD),
            preferred_element_type=jnp.float32,
        )
        * score_scale
    )
    final_max = jnp.maximum(row_max, own_score)
    old_factor = jnp.exp(row_max - final_max)
    own_weight = jnp.exp(own_score - final_max)
    row_total = row_total * old_factor + own_weight
    own_rounded = lax.optimization_barrier(own_weight.astype(jnp.bfloat16)).astype(jnp.float32)
    fresh_value = new_value.reshape(sessions, local_heads, 1, HD).astype(jnp.float32)
    weighted = weighted * old_factor[..., None] + own_rounded[..., None] * fresh_value
    decode_attended = (weighted / row_total[..., None]).reshape(sessions, -1).astype(jnp.bfloat16)
    return (prompt_attended, decode_attended)


MESH = pl.DeviceIdType.MESH
LOW = -1e30
FAR = 1 << 30


def pick(index, table):
    out = jnp.int32(table[0])
    for i in range(1, len(table)):
        out = jnp.where(index == i, jnp.int32(table[i]), out)
    return out


def fused_kernel(
    outer, inner, cores,
    pq_hbm, pk_hbm, pv_hbm, length_ref, order_ref, nq_hbm, nk_hbm, nv_hbm, ck_hbm, cv_hbm, clen_ref,
    out_ref, dec_ref,
    pq, kbuf, vbuf, ck, cv, nq_ref, nk_ref, nv_ref, qrows, sum_out, sum_in, stat_out, stat_in,
    done, flat,
    in_sem, kv_send, kv_recv, part_send, part_recv, done_send, done_recv,
):
    group = QH // KVH
    span = kbuf.shape[1] // (inner * cores)
    n_seq = outer * inner
    seq = lax.axis_index("seq")
    core = lax.axis_index("head")
    a = seq // inner
    b = seq % inner
    log2_scale = math.log2(math.e) / math.sqrt(HD)

    def rows_of(b_, c_):
        return pl.ds(pl.multiple_of((b_ * cores + c_) * span, span), span)

    def block_id(a_, b_, c_):
        return (a_ * inner + b_) * cores + c_

    local = [
        pltpu.make_async_copy(pk_hbm, kbuf.at[a, rows_of(b, core)], in_sem.at[0]),
        pltpu.make_async_copy(pv_hbm, vbuf.at[a, rows_of(b, core)], in_sem.at[1]),
        pltpu.make_async_copy(ck_hbm, ck, in_sem.at[2]),
        pltpu.make_async_copy(cv_hbm, cv, in_sem.at[3]),
        pltpu.make_async_copy(pq_hbm, pq, in_sem.at[4]),
        pltpu.make_async_copy(nq_hbm, nq_ref, in_sem.at[5]),
        pltpu.make_async_copy(nk_hbm, nk_ref, in_sem.at[6]),
        pltpu.make_async_copy(nv_hbm, nv_ref, in_sem.at[7]),
    ]
    for copy in local:
        copy.start()

    barrier = pltpu.get_barrier_semaphore()
    for d in range(1, n_seq):
        pl.semaphore_signal(
            barrier, inc=1, device_id={"seq": (seq + d) % n_seq}, device_id_type=MESH
        )
    for d in range(1, cores):
        pl.semaphore_signal(
            barrier, inc=1, device_id={"head": (core + d) % cores}, device_id_type=MESH
        )
    local[0].wait()
    local[1].wait()
    pl.semaphore_wait(barrier, n_seq - 1 + cores - 1)

    sends = []

    bufs = (kbuf, vbuf)

    def send(which, a_, b_, c_, target):
        ref = bufs[which].at[a_, rows_of(b_, c_)]
        copy = pltpu.make_async_remote_copy(
            src_ref=ref,
            dst_ref=ref,
            send_sem=kv_send.at[len(sends)],
            recv_sem=kv_recv.at[which, block_id(a_, b_, c_)],
            device_id=target,
            device_id_type=MESH,
        )
        copy.start()
        sends.append(copy)

    def await_block(which, a_, b_, c_):
        ref = bufs[which].at[a_, rows_of(b_, c_)]
        pltpu.make_async_remote_copy(
            src_ref=ref,
            dst_ref=ref,
            send_sem=kv_send.at[0],
            recv_sem=kv_recv.at[which, block_id(a_, b_, c_)],
            device_id={"seq": seq},
            device_id_type=MESH,
        ).wait_recv()

    def to_inner(which, a_, b_, c_):
        for d in range(1, inner):
            send(which, a_, b_, c_, {"seq": a * inner + (b + d) % inner})

    def to_core(which, a_, b_, c_):
        for d in range(1, cores):
            send(which, a_, b_, c_, {"head": (core + d) % cores})

    nearest = [sorted(range(outer), key=lambda p, i=i: (abs(p - i), p)) for i in range(outer)]
    planes = [pick(a, [nearest[i][k] for i in range(outer)]) for k in range(outer)]

    for which in range(2):
        to_inner(which, a, b, core)
        if outer > 1:
            send(which, a, b, core, {"seq": planes[1] * inner + b})
    for k in range(2, outer):
        for which in range(2):
            send(which, a, b, core, {"seq": planes[k] * inner + b})
    for which in range(2):
        to_core(which, a, b, core)

    sessions, ctx = ck.shape[0], ck.shape[2]
    per = sessions // n_seq
    field = HD // (2 * per)
    for copy in local[5:]:
        copy.wait()
    for h in range(8):
        if h < group:
            qrows[pl.ds(h * sessions, sessions), :] = nq_ref[:, h * HD : (h + 1) * HD].astype(
                jnp.float32
            )
        else:
            qrows[pl.ds(h * sessions, sessions), :] = jnp.zeros((sessions, HD), jnp.float32)
    local[2].wait()
    local[3].wait()
    cache_pos = seq * ctx + lax.broadcasted_iota(jnp.int32, (8, ctx), 1)
    first = seq == 0
    nk = nk_ref[...].astype(jnp.float32)
    nv = nv_ref[...].astype(jnp.float32)
    inv = 1.0 / math.sqrt(HD)
    for s in range(sessions):
        q32 = qrows[pl.ds(s, 8, stride=sessions), :]
        sc = lax.dot_general(
            q32.astype(jnp.bfloat16), ck[s, 0], (((1,), (1,)), ((), ())),
            preferred_element_type=jnp.float32,
        ) * inv
        own = jnp.sum(q32 * nk[s : s + 1, :], axis=1, keepdims=True) * inv
        own = jnp.where(first, own, LOW)
        valid = cache_pos < clen_ref[s]
        sc = jnp.where(valid, sc, LOW)
        top = jnp.maximum(jnp.max(sc, axis=1, keepdims=True), own)
        w = jnp.where(valid, jnp.exp(sc - top), 0.0)
        own_w = jnp.where(first, jnp.exp(own - top), 0.0)
        tot = jnp.sum(w, axis=1, keepdims=True) + own_w
        o = jnp.dot(w.astype(jnp.bfloat16), cv[s, 0], preferred_element_type=jnp.float32)
        o = o + own_w.astype(jnp.bfloat16).astype(jnp.float32) * nv[s : s + 1, :]
        lane = lax.broadcasted_iota(jnp.int32, (8, HD), 1)
        dst, at = s // per, s % per
        if at == 0:
            outs, stats = [], jnp.zeros((8, HD), jnp.float32)
        outs.append(o)
        stats = jnp.where(lane // field == 2 * at, top, stats)
        stats = jnp.where(lane // field == 2 * at + 1, tot, stats)
        if at == per - 1:
            sum_out[dst] = jnp.concatenate(outs, axis=0).astype(jnp.bfloat16)
            stat_out[dst] = stats

    part_copies = []
    for d in range(1, n_seq):
        peer = (seq + d) % n_seq
        for which, out, into in ((0, stat_out, stat_in), (1, sum_out, sum_in)):
            copy = pltpu.make_async_remote_copy(
                src_ref=out.at[peer],
                dst_ref=into.at[n_seq - 1 - d],
                send_sem=part_send.at[which, d - 1],
                recv_sem=part_recv.at[which, n_seq - 1 - d],
                device_id={"seq": peer},
                device_id_type=MESH,
            )
            copy.start()
            part_copies.append(copy)

    local[4].wait()
    me_block = block_id(a, b, core)
    limit = length_ref[0]
    rows = group * span
    row_pos = order_ref[me_block] * span + lax.broadcasted_iota(jnp.int32, (rows, 1), 0) % span
    keys = kbuf.shape[1]
    lane = lax.broadcasted_iota(jnp.int32, (1, keys), 1)
    queries = [
        jnp.concatenate(
            [pq[:, (g * group + h) * HD : (g * group + h + 1) * HD] for h in range(group)], axis=0
        )
        for g in range(KVH)
    ]
    state = [None] * KVH

    def attend(a_):
        base = jnp.zeros((1, keys), jnp.int32)
        for j in range(inner * cores):
            base = jnp.where(lane // span == j, order_ref[a_ * inner * cores + j], base)
        key_pos = base * span + lane % span
        key_pos = jnp.where(key_pos < limit, key_pos, FAR)
        allowed = key_pos <= row_pos
        for g in range(KVH):
            kk = kbuf[a_, :, g * HD : (g + 1) * HD]
            vv = vbuf[a_, :, g * HD : (g + 1) * HD]
            sc = lax.dot_general(
                queries[g], kk, (((1,), (1,)), ((), ())), preferred_element_type=jnp.float32
            )
            sc = jnp.where(allowed, sc, LOW)
            best = jnp.max(sc, axis=1, keepdims=True)
            if state[g] is not None:
                best = jnp.maximum(best, state[g][0])
            w = jnp.exp2((sc - best) * log2_scale)
            tot = jnp.sum(w, axis=1, keepdims=True)
            o = jnp.dot(w.astype(jnp.bfloat16), vv, preferred_element_type=jnp.float32)
            if state[g] is not None:
                old, old_tot, old_o = state[g]
                f = jnp.exp2((old - best) * log2_scale)
                tot = tot + old_tot * f
                o = o + old_o * f
            state[g] = (best, tot, o)

    def decode_combine():
        for k in range(n_seq - 1):
            for which, out, into in ((0, stat_out, stat_in), (1, sum_out, sum_in)):
                pltpu.make_async_remote_copy(
                    src_ref=out.at[0],
                    dst_ref=into.at[k],
                    send_sem=part_send.at[which, 0],
                    recv_sem=part_recv.at[which, k],
                    device_id={"seq": seq},
                    device_id_type=MESH,
                ).wait_recv()
        stats = [stat_out[seq]] + [stat_in[k] for k in range(n_seq - 1)]
        sums = [sum_out[seq]] + [sum_in[k] for k in range(n_seq - 1)]

        def spread(which):
            return [
                jnp.concatenate(
                    [
                        x[:, (2 * at + which) * field : (2 * at + which) * field + 1]
                        for at in range(per)
                    ],
                    axis=0,
                )
                for x in stats
            ]

        tops, tots = spread(0), spread(1)
        top = functools.reduce(jnp.maximum, tops)
        fs = [jnp.exp(t - top) for t in tops]
        tot = sum(f * t for f, t in zip(fs, tots))
        o = sum(f * x.astype(jnp.float32) for f, x in zip(fs, sums))
        done[seq] = (o / tot).astype(jnp.bfloat16)
        copies = []
        for d in range(1, n_seq):
            peer = (seq + d) % n_seq
            copy = pltpu.make_async_remote_copy(
                src_ref=done.at[seq],
                dst_ref=done.at[seq],
                send_sem=done_send.at[d - 1],
                recv_sem=done_recv.at[seq],
                device_id={"seq": peer},
                device_id_type=MESH,
            )
            copy.start()
            copies.append(copy)
        return copies

    done_copies = []
    for k in range(outer):
        if k + 1 < outer:
            for which in range(2):
                await_block(which, planes[k + 1], b, core)
                to_inner(which, planes[k + 1], b, core)
                to_core(which, planes[k + 1], b, core)
        for which in range(2):
            for d in range(1, inner):
                await_block(which, planes[k], (b + d) % inner, core)
                to_core(which, planes[k], (b + d) % inner, core)
        if k == max(outer - 2, 0):
            done_copies = decode_combine()
        for d in range(1, cores):
            for d2 in range(inner):
                for which in range(2):
                    await_block(which, planes[k], (b + d2) % inner, (core + d) % cores)
        attend(planes[k])

    live = row_pos < limit
    for g in range(KVH):
        _, tot, o = state[g]
        res = jnp.where(live, o / tot, 0.0).astype(jnp.bfloat16)
        for h in range(group):
            out_ref[:, (g * group + h) * HD : (g * group + h + 1) * HD] = res[
                h * span : (h + 1) * span
            ]

    for d in range(1, n_seq):
        peer = (seq + d) % n_seq
        pltpu.make_async_remote_copy(
            src_ref=done.at[peer],
            dst_ref=done.at[peer],
            send_sem=done_send.at[0],
            recv_sem=done_recv.at[peer],
            device_id={"seq": seq},
            device_id_type=MESH,
        ).wait_recv()
    flat[...] = done[...].reshape(flat.shape).astype(jnp.float32)
    for h in range(group):
        dec_ref[:, h * HD : (h + 1) * HD] = flat[pl.ds(h, sessions, stride=8), :].astype(
            jnp.bfloat16
        )
    for copy in sends + part_copies + done_copies:
        copy.wait_send()


def store_kernel(prompt_ref, decode_ref, prompt_out, decode_out, sem):
    copies = [
        pltpu.make_async_copy(prompt_ref, prompt_out, sem.at[0]),
        pltpu.make_async_copy(decode_ref, decode_out, sem.at[1]),
    ]
    for copy in copies:
        copy.start()
    for copy in copies:
        copy.wait()


def fused(outer, inner, cores, *args):
    pq, pk, pv, length, order, nq, nk, nv, ck, cv, clen = args
    span = pq.shape[0]
    sessions = nq.shape[0]
    n_seq = outer * inner
    per = sessions // n_seq
    n_sends = (outer - 1) + outer * (inner - 1) + n_seq * (cores - 1)
    keys = inner * cores * span
    hbm = pl.BlockSpec(memory_space=pltpu.HBM)
    vmem = pl.BlockSpec(memory_space=pltpu.VMEM)
    smem = pl.BlockSpec(memory_space=pltpu.SMEM)
    dma = pltpu.SemaphoreType.DMA
    results = pl.pallas_call(
        functools.partial(fused_kernel, outer, inner, cores),
        name="attention",
        out_shape=(
            jax.ShapeDtypeStruct(pq.shape, jnp.bfloat16),
            jax.ShapeDtypeStruct(nq.shape, jnp.bfloat16),
        ),
        in_specs=[hbm, hbm, hbm, smem, smem, hbm, hbm, hbm, hbm, hbm, smem],
        out_specs=(vmem, vmem),
        scratch_shapes=[
            pltpu.VMEM(pq.shape, jnp.bfloat16),
            pltpu.VMEM((outer, keys, pk.shape[1]), jnp.bfloat16),
            pltpu.VMEM((outer, keys, pv.shape[1]), jnp.bfloat16),
            pltpu.VMEM(ck.shape, jnp.bfloat16),
            pltpu.VMEM(cv.shape, jnp.bfloat16),
            pltpu.VMEM(nq.shape, jnp.bfloat16),
            pltpu.VMEM(nk.shape, jnp.bfloat16),
            pltpu.VMEM(nv.shape, jnp.bfloat16),
            pltpu.VMEM((8 * sessions, HD), jnp.float32),
            pltpu.VMEM((n_seq, per * 8, HD), jnp.bfloat16),
            pltpu.VMEM((n_seq - 1, per * 8, HD), jnp.bfloat16),
            pltpu.VMEM((n_seq, 8, HD), jnp.float32),
            pltpu.VMEM((n_seq - 1, 8, HD), jnp.float32),
            pltpu.VMEM((n_seq, per * 8, HD), jnp.bfloat16),
            pltpu.VMEM((8 * sessions, HD), jnp.float32),
            dma((8,)),
            dma((2 * n_sends,)),
            dma((2, n_seq * cores)),
            dma((2, n_seq - 1)),
            dma((2, n_seq - 1)),
            dma((n_seq - 1,)),
            dma((n_seq,)),
        ],
        compiler_params=pltpu.CompilerParams(
            collective_id=0, has_side_effects=True, vmem_limit_bytes=48 * 1024 * 1024
        ),
    )(
        *(
            x if x.dtype == jnp.int32 else pltpu.with_memory_space_constraint(x, pltpu.HBM)
            for x in args
        )
    )
    return pl.pallas_call(
        store_kernel,
        name="store",
        out_shape=tuple(jax.ShapeDtypeStruct(x.shape, x.dtype) for x in results),
        in_specs=[pl.BlockSpec(memory_space=pl.ANY)] * 2,
        out_specs=(pl.BlockSpec(memory_space=pl.ANY),) * 2,
        scratch_shapes=[dma((2,))],
        compiler_params=pltpu.CompilerParams(vmem_limit_bytes=4 * 1024 * 1024),
    )(*results)


def per_device(outer, inner, cores, *args):
    sessions, span = args[5].shape[0], args[0].shape[0]
    if sessions % (outer * inner) or span % 16 or QH // KVH > 8:
        return composed(*args)
    return fused(outer, inner, cores, *args)


def solution(mesh):
    n_seq, cores = mesh.shape["seq"], mesh.shape["head"]
    inner = max(d for d in range(1, math.isqrt(n_seq) + 1) if n_seq % d == 0)
    return jax.shard_map(
        functools.partial(per_device, n_seq // inner, inner, cores),
        mesh=mesh,
        in_specs=(
            P(("rep", "seq", "head"), None),
            P(("rep", "seq", "head"), None),
            P(("rep", "seq", "head"), None),
            P("rep"),
            P("rep"),
            P("rep", "head"),
            P("rep", "head"),
            P("rep", "head"),
            P("rep", "head", "seq", None),
            P("rep", "head", "seq", None),
            P("rep"),
        ),
        out_specs=(P(("rep", "seq", "head"), None), P("rep", "head")),
        check_vma=False,
    )
```

```python
import functools
import math

import jax
import jax.numpy as jnp
from jax import lax
from jax.experimental import pallas as pl
from jax.experimental.pallas import tpu as pltpu
from jax.sharding import PartitionSpec as P

HD = 128
QH = 14
KVH = 2


def lookup(span_table, row_ids, span_rows):
    chosen = (
        row_ids[:, None] // span_rows == jnp.arange(span_table.shape[0], dtype=jnp.int32)[None, :]
    )
    picked = jnp.sum(jnp.where(chosen, span_table[None, :], 0), axis=1)
    return picked * span_rows + row_ids % span_rows


def block_size(key_count, span_rows):
    units = key_count // span_rows
    most = max(1, 512 // span_rows)
    best = 1
    for count in range(1, min(units, most) + 1):
        if units % count == 0:
            best = count
    return best * span_rows


def start_state(query_rows, kv_heads, head_group):
    row_max = jnp.full((kv_heads, head_group, query_rows), -1e30, jnp.float32)
    row_total = jnp.zeros((kv_heads, head_group, query_rows), jnp.float32)
    weighted = jnp.zeros((kv_heads, head_group, query_rows, HD), jnp.float32)
    return (row_max, row_total, weighted)


def attend_rows(running, shard_piece, queries, query_pos, span_table, span_rows, length_limit):
    keys_piece, values_piece = shard_piece
    key_count = keys_piece.shape[0]
    kv_heads = queries.shape[1]
    block_rows = block_size(key_count, span_rows)
    score_scale = 1.0 / math.sqrt(HD)

    def advance(carried, block_index):
        first_row = block_index * block_rows
        key_block = lax.dynamic_slice_in_dim(keys_piece, first_row, block_rows, 0).reshape(
            block_rows, kv_heads, HD
        )
        value_block = lax.dynamic_slice_in_dim(values_piece, first_row, block_rows, 0).reshape(
            block_rows, kv_heads, HD
        )
        key_pos = lookup(span_table, first_row + jnp.arange(block_rows, dtype=jnp.int32), span_rows)
        allowed = (key_pos[None, :] <= query_pos[:, None]) & (key_pos[None, :] < length_limit)

        def compute(state_in):
            row_max, row_total, weighted = state_in
            scores = (
                jnp.einsum("rkgd,nkd->kgrn", queries, key_block, preferred_element_type=jnp.float32)
                * score_scale
            )
            scores = jnp.where(allowed, scores, -1e30)
            new_max = jnp.maximum(row_max, jnp.max(scores, axis=-1))
            weights = jnp.where(allowed, jnp.exp(scores - new_max[..., None]), 0.0)
            factor = jnp.exp(row_max - new_max)
            row_total = row_total * factor + jnp.sum(weights, axis=-1)
            weighted = weighted * factor[..., None] + jnp.einsum(
                "kgrn,nkd->kgrd",
                weights.astype(jnp.bfloat16),
                value_block,
                preferred_element_type=jnp.float32,
            )
            return (new_max, row_total, weighted)

        return (lax.cond(jnp.any(allowed), compute, lambda state_in: state_in, carried), None)

    running, _ = lax.scan(advance, running, jnp.arange(key_count // block_rows, dtype=jnp.int32))
    return running


def finish(running, query_pos, length_limit):
    row_max, row_total, weighted = running
    result = weighted / row_total[..., None]
    result = jnp.transpose(result, (2, 0, 1, 3))
    result = jnp.where((query_pos < length_limit)[:, None, None, None], result, 0.0)
    return result.reshape(result.shape[0], -1).astype(jnp.bfloat16)


def composed(
    prompt_query,
    prompt_key,
    prompt_value,
    prompt_length,
    span_order,
    new_query,
    new_key,
    new_value,
    cache_key,
    cache_value,
    cache_length,
):
    head_group = QH // KVH
    score_scale = 1.0 / math.sqrt(HD)
    length_limit = prompt_length[0]
    span_rows = prompt_query.shape[0]
    kv_heads = prompt_key.shape[1] // HD
    first_row = (lax.axis_index("seq") * lax.axis_size("head") + lax.axis_index("head")) * span_rows
    query_pos = lookup(span_order, first_row + jnp.arange(span_rows, dtype=jnp.int32), span_rows)
    queries = prompt_query.reshape(span_rows, kv_heads, head_group, HD)
    running = attend_rows(
        start_state(span_rows, kv_heads, head_group),
        (
            lax.all_gather(prompt_key, ("seq", "head"), axis=0, tiled=True),
            lax.all_gather(prompt_value, ("seq", "head"), axis=0, tiled=True),
        ),
        queries,
        query_pos,
        span_order,
        span_rows,
        length_limit,
    )
    prompt_attended = finish(running, query_pos, length_limit)
    sessions = new_query.shape[0]
    local_heads = cache_key.shape[1]
    local_ctx = cache_key.shape[2]
    dec_queries = new_query.reshape(sessions, local_heads, head_group, HD)
    cache_pos = lax.axis_index("seq") * local_ctx + jnp.arange(local_ctx, dtype=jnp.int32)
    valid = (cache_pos[None, :] < cache_length[:, None])[:, None, None, :]
    scores = (
        jnp.einsum("skgd,sktd->skgt", dec_queries, cache_key, preferred_element_type=jnp.float32)
        * score_scale
    )
    scores = jnp.where(valid, scores, -1e30)
    row_max = jnp.max(scores, axis=-1)
    weights = jnp.where(valid, jnp.exp(scores - row_max[..., None]), 0.0)
    row_total = jnp.sum(weights, axis=-1)
    weighted = jnp.einsum(
        "skgt,sktd->skgd",
        weights.astype(jnp.bfloat16),
        cache_value,
        preferred_element_type=jnp.float32,
    )
    global_max = lax.pmax(row_max, "seq")
    factor = jnp.exp(row_max - global_max)
    row_total, weighted = lax.psum((row_total * factor, weighted * factor[..., None]), "seq")
    row_max = global_max
    own_score = (
        jnp.einsum(
            "skgd,skd->skg",
            dec_queries,
            new_key.reshape(sessions, local_heads, HD),
            preferred_element_type=jnp.float32,
        )
        * score_scale
    )
    final_max = jnp.maximum(row_max, own_score)
    old_factor = jnp.exp(row_max - final_max)
    own_weight = jnp.exp(own_score - final_max)
    row_total = row_total * old_factor + own_weight
    own_rounded = lax.optimization_barrier(own_weight.astype(jnp.bfloat16)).astype(jnp.float32)
    fresh_value = new_value.reshape(sessions, local_heads, 1, HD).astype(jnp.float32)
    weighted = weighted * old_factor[..., None] + own_rounded[..., None] * fresh_value
    decode_attended = (weighted / row_total[..., None]).reshape(sessions, -1).astype(jnp.bfloat16)
    return (prompt_attended, decode_attended)


MESH = pl.DeviceIdType.MESH
LOW = -1e30
FAR = 1 << 30


def pick(index, table):
    out = jnp.int32(table[0])
    for i in range(1, len(table)):
        out = jnp.where(index == i, jnp.int32(table[i]), out)
    return out


def fused_kernel(
    outer, inner, cores,
    pq_hbm, pk_hbm, pv_hbm, length_ref, order_ref, nq_hbm, nk_hbm, nv_hbm, ck_hbm, cv_hbm, clen_ref,
    out_ref, dec_ref,
    pq, kbuf, vbuf, ck, cv, nq_ref, nk_ref, nv_ref, qrows, sum_out, sum_in, stat_out, stat_in,
    done, flat,
    in_sem, kv_send, kv_recv, part_send, part_recv, done_send, done_recv, hello,
):
    group = QH // KVH
    span = kbuf.shape[1] // (inner * cores)
    n_seq = outer * inner
    seq = lax.axis_index("seq")
    core = lax.axis_index("head")
    a = seq // inner
    b = seq % inner
    log2_scale = math.log2(math.e) / math.sqrt(HD)

    def rows_of(b_, c_):
        return pl.ds(pl.multiple_of((b_ * cores + c_) * span, span), span)

    def block_id(a_, b_, c_):
        return (a_ * inner + b_) * cores + c_

    local = [
        pltpu.make_async_copy(pk_hbm, kbuf.at[a, rows_of(b, core)], in_sem.at[0]),
        pltpu.make_async_copy(pv_hbm, vbuf.at[a, rows_of(b, core)], in_sem.at[1]),
        pltpu.make_async_copy(ck_hbm, ck, in_sem.at[2]),
        pltpu.make_async_copy(cv_hbm, cv, in_sem.at[3]),
        pltpu.make_async_copy(pq_hbm, pq, in_sem.at[4]),
        pltpu.make_async_copy(nq_hbm, nq_ref, in_sem.at[5]),
        pltpu.make_async_copy(nk_hbm, nk_ref, in_sem.at[6]),
        pltpu.make_async_copy(nv_hbm, nv_ref, in_sem.at[7]),
    ]
    for copy in local:
        copy.start()

    barrier = pltpu.get_barrier_semaphore()

    def greet_line(sem):
        for step, there in ((-1, a > 0), (1, a < outer - 1)):

            @pl.when(there)
            def _(step=step):
                pl.semaphore_signal(
                    sem, inc=1, device_id={"seq": seq + step * inner}, device_id_type=MESH
                )

    def greet_inner(sem):
        for d in range(1, inner):
            pl.semaphore_signal(
                sem,
                inc=1,
                device_id={"seq": a * inner + (b + d) % inner},
                device_id_type=MESH,
            )

    beside = jnp.where(a > 0, 1, 0) + jnp.where(a < outer - 1, 1, 0)
    greet_line(barrier)
    greet_inner(barrier)
    for d in range(1, cores):
        pl.semaphore_signal(
            barrier, inc=1, device_id={"head": (core + d) % cores}, device_id_type=MESH
        )
    local[0].wait()
    local[1].wait()
    pl.semaphore_wait(barrier, beside + inner - 1 + cores - 1)

    sends = []

    bufs = (kbuf, vbuf)

    def send(which, a_, b_, c_, target):
        ref = bufs[which].at[a_, rows_of(b_, c_)]
        copy = pltpu.make_async_remote_copy(
            src_ref=ref,
            dst_ref=ref,
            send_sem=kv_send.at[len(sends)],
            recv_sem=kv_recv.at[which, block_id(a_, b_, c_)],
            device_id=target,
            device_id_type=MESH,
        )
        copy.start()
        sends.append(copy)

    def await_block(which, a_, b_, c_):
        ref = bufs[which].at[a_, rows_of(b_, c_)]
        pltpu.make_async_remote_copy(
            src_ref=ref,
            dst_ref=ref,
            send_sem=kv_send.at[0],
            recv_sem=kv_recv.at[which, block_id(a_, b_, c_)],
            device_id={"seq": seq},
            device_id_type=MESH,
        ).wait_recv()

    def to_inner(which, a_, b_, c_):
        for d in range(1, inner):
            send(which, a_, b_, c_, {"seq": a * inner + (b + d) % inner})

    def to_core(which, a_, b_, c_):
        for d in range(1, cores):
            send(which, a_, b_, c_, {"head": (core + d) % cores})

    nearest = [sorted(range(outer), key=lambda p, i=i: (abs(p - i), abs(2 * p - outer + 1))) for i in range(outer)]
    planes = [pick(a, [nearest[i][k] for i in range(outer)]) for k in range(outer)]

    for which in range(2):
        to_inner(which, a, b, core)
        if outer > 1:
            send(which, a, b, core, {"seq": planes[1] * inner + b})
    for r in range(outer - 2):
        greet_line(hello.at[r])
        pl.semaphore_wait(hello.at[r], beside)
    greet_inner(hello.at[outer - 1])
    for k in range(2, outer):
        for which in range(2):
            send(which, a, b, core, {"seq": planes[k] * inner + b})
    for which in range(2):
        to_core(which, a, b, core)

    sessions, ctx = ck.shape[0], ck.shape[2]
    per = sessions // n_seq
    field = HD // (2 * per)
    for copy in local[5:]:
        copy.wait()
    for h in range(8):
        if h < group:
            qrows[pl.ds(h * sessions, sessions), :] = nq_ref[:, h * HD : (h + 1) * HD].astype(
                jnp.float32
            )
        else:
            qrows[pl.ds(h * sessions, sessions), :] = jnp.zeros((sessions, HD), jnp.float32)
    local[2].wait()
    local[3].wait()
    cache_pos = seq * ctx + lax.broadcasted_iota(jnp.int32, (8, ctx), 1)
    first = seq == 0
    nk = nk_ref[...].astype(jnp.float32)
    nv = nv_ref[...].astype(jnp.float32)
    inv = 1.0 / math.sqrt(HD)
    for s in range(sessions):
        q32 = qrows[pl.ds(s, 8, stride=sessions), :]
        sc = lax.dot_general(
            q32.astype(jnp.bfloat16), ck[s, 0], (((1,), (1,)), ((), ())),
            preferred_element_type=jnp.float32,
        ) * inv
        own = jnp.sum(q32 * nk[s : s + 1, :], axis=1, keepdims=True) * inv
        own = jnp.where(first, own, LOW)
        valid = cache_pos < clen_ref[s]
        sc = jnp.where(valid, sc, LOW)
        top = jnp.maximum(jnp.max(sc, axis=1, keepdims=True), own)
        w = jnp.where(valid, jnp.exp(sc - top), 0.0)
        own_w = jnp.where(first, jnp.exp(own - top), 0.0)
        tot = jnp.sum(w, axis=1, keepdims=True) + own_w
        o = jnp.dot(w.astype(jnp.bfloat16), cv[s, 0], preferred_element_type=jnp.float32)
        o = o + own_w.astype(jnp.bfloat16).astype(jnp.float32) * nv[s : s + 1, :]
        lane = lax.broadcasted_iota(jnp.int32, (8, HD), 1)
        dst, at = s // per, s % per
        if at == 0:
            outs, stats = [], jnp.zeros((8, HD), jnp.float32)
        outs.append(o)
        stats = jnp.where(lane // field == 2 * at, top, stats)
        stats = jnp.where(lane // field == 2 * at + 1, tot, stats)
        if at == per - 1:
            sum_out[dst] = jnp.concatenate(outs, axis=0).astype(jnp.bfloat16)
            stat_out[dst] = stats

    pl.semaphore_wait(hello.at[outer - 1], inner - 1)
    part_copies = []
    for d in range(1, n_seq):
        peer = (seq + d) % n_seq
        for which, out, into in ((0, stat_out, stat_in), (1, sum_out, sum_in)):
            copy = pltpu.make_async_remote_copy(
                src_ref=out.at[peer],
                dst_ref=into.at[n_seq - 1 - d],
                send_sem=part_send.at[which, d - 1],
                recv_sem=part_recv.at[which, n_seq - 1 - d],
                device_id={"seq": peer},
                device_id_type=MESH,
            )
            copy.start()
            part_copies.append(copy)

    local[4].wait()
    me_block = block_id(a, b, core)
    limit = length_ref[0]
    rows = group * span
    row_pos = order_ref[me_block] * span + lax.broadcasted_iota(jnp.int32, (rows, 1), 0) % span
    keys = kbuf.shape[1]
    lane = lax.broadcasted_iota(jnp.int32, (1, keys), 1)
    queries = [
        jnp.concatenate(
            [pq[:, (g * group + h) * HD : (g * group + h + 1) * HD] for h in range(group)], axis=0
        )
        for g in range(KVH)
    ]
    state = [None] * KVH

    def attend(a_):
        base = jnp.zeros((1, keys), jnp.int32)
        for j in range(inner * cores):
            base = jnp.where(lane // span == j, order_ref[a_ * inner * cores + j], base)
        key_pos = base * span + lane % span
        key_pos = jnp.where(key_pos < limit, key_pos, FAR)
        allowed = key_pos <= row_pos
        for g in range(KVH):
            kk = kbuf[a_, :, g * HD : (g + 1) * HD]
            vv = vbuf[a_, :, g * HD : (g + 1) * HD]
            sc = lax.dot_general(
                queries[g], kk, (((1,), (1,)), ((), ())), preferred_element_type=jnp.float32
            )
            sc = jnp.where(allowed, sc, LOW)
            best = jnp.max(sc, axis=1, keepdims=True)
            if state[g] is not None:
                best = jnp.maximum(best, state[g][0])
            w = jnp.exp2((sc - best) * log2_scale)
            tot = jnp.sum(w, axis=1, keepdims=True)
            o = jnp.dot(w.astype(jnp.bfloat16), vv, preferred_element_type=jnp.float32)
            if state[g] is not None:
                old, old_tot, old_o = state[g]
                f = jnp.exp2((old - best) * log2_scale)
                tot = tot + old_tot * f
                o = o + old_o * f
            state[g] = (best, tot, o)

    def decode_combine():
        for k in range(n_seq - 1):
            for which, out, into in ((0, stat_out, stat_in), (1, sum_out, sum_in)):
                pltpu.make_async_remote_copy(
                    src_ref=out.at[0],
                    dst_ref=into.at[k],
                    send_sem=part_send.at[which, 0],
                    recv_sem=part_recv.at[which, k],
                    device_id={"seq": seq},
                    device_id_type=MESH,
                ).wait_recv()
        stats = [stat_out[seq]] + [stat_in[k] for k in range(n_seq - 1)]
        sums = [sum_out[seq]] + [sum_in[k] for k in range(n_seq - 1)]

        def spread(which):
            return [
                jnp.concatenate(
                    [
                        x[:, (2 * at + which) * field : (2 * at + which) * field + 1]
                        for at in range(per)
                    ],
                    axis=0,
                )
                for x in stats
            ]

        tops, tots = spread(0), spread(1)
        top = functools.reduce(jnp.maximum, tops)
        fs = [jnp.exp(t - top) for t in tops]
        tot = sum(f * t for f, t in zip(fs, tots))
        o = sum(f * x.astype(jnp.float32) for f, x in zip(fs, sums))
        done[seq] = (o / tot).astype(jnp.bfloat16)
        copies = []
        for d in range(1, n_seq):
            peer = (seq + d) % n_seq
            copy = pltpu.make_async_remote_copy(
                src_ref=done.at[seq],
                dst_ref=done.at[seq],
                send_sem=done_send.at[d - 1],
                recv_sem=done_recv.at[seq],
                device_id={"seq": peer},
                device_id_type=MESH,
            )
            copy.start()
            copies.append(copy)
        return copies

    done_copies = []
    for k in range(outer):
        if k + 1 < outer:
            for which in range(2):
                await_block(which, planes[k + 1], b, core)
                to_inner(which, planes[k + 1], b, core)
                to_core(which, planes[k + 1], b, core)
        for which in range(2):
            for d in range(1, inner):
                await_block(which, planes[k], (b + d) % inner, core)
                to_core(which, planes[k], (b + d) % inner, core)
        if k == max(outer - 2, 0):
            done_copies = decode_combine()
        for d in range(1, cores):
            for d2 in range(inner):
                for which in range(2):
                    await_block(which, planes[k], (b + d2) % inner, (core + d) % cores)
        attend(planes[k])

    live = row_pos < limit
    for g in range(KVH):
        _, tot, o = state[g]
        res = jnp.where(live, o / tot, 0.0).astype(jnp.bfloat16)
        for h in range(group):
            out_ref[:, (g * group + h) * HD : (g * group + h + 1) * HD] = res[
                h * span : (h + 1) * span
            ]

    for d in range(1, n_seq):
        peer = (seq + d) % n_seq
        pltpu.make_async_remote_copy(
            src_ref=done.at[peer],
            dst_ref=done.at[peer],
            send_sem=done_send.at[0],
            recv_sem=done_recv.at[peer],
            device_id={"seq": seq},
            device_id_type=MESH,
        ).wait_recv()
    flat[...] = done[...].reshape(flat.shape).astype(jnp.float32)
    for h in range(group):
        dec_ref[:, h * HD : (h + 1) * HD] = flat[pl.ds(h, sessions, stride=8), :].astype(
            jnp.bfloat16
        )
    for copy in sends + part_copies + done_copies:
        copy.wait_send()


def store_kernel(prompt_ref, decode_ref, prompt_out, decode_out, sem):
    copies = [
        pltpu.make_async_copy(prompt_ref, prompt_out, sem.at[0]),
        pltpu.make_async_copy(decode_ref, decode_out, sem.at[1]),
    ]
    for copy in copies:
        copy.start()
    for copy in copies:
        copy.wait()


def fused(outer, inner, cores, *args):
    pq, pk, pv, length, order, nq, nk, nv, ck, cv, clen = args
    span = pq.shape[0]
    sessions = nq.shape[0]
    n_seq = outer * inner
    per = sessions // n_seq
    n_sends = (outer - 1) + outer * (inner - 1) + n_seq * (cores - 1)
    keys = inner * cores * span
    hbm = pl.BlockSpec(memory_space=pltpu.HBM)
    vmem = pl.BlockSpec(memory_space=pltpu.VMEM)
    smem = pl.BlockSpec(memory_space=pltpu.SMEM)
    dma = pltpu.SemaphoreType.DMA
    results = pl.pallas_call(
        functools.partial(fused_kernel, outer, inner, cores),
        name="attention",
        out_shape=(
            jax.ShapeDtypeStruct(pq.shape, jnp.bfloat16),
            jax.ShapeDtypeStruct(nq.shape, jnp.bfloat16),
        ),
        in_specs=[hbm, hbm, hbm, smem, smem, hbm, hbm, hbm, hbm, hbm, smem],
        out_specs=(vmem, vmem),
        scratch_shapes=[
            pltpu.VMEM(pq.shape, jnp.bfloat16),
            pltpu.VMEM((outer, keys, pk.shape[1]), jnp.bfloat16),
            pltpu.VMEM((outer, keys, pv.shape[1]), jnp.bfloat16),
            pltpu.VMEM(ck.shape, jnp.bfloat16),
            pltpu.VMEM(cv.shape, jnp.bfloat16),
            pltpu.VMEM(nq.shape, jnp.bfloat16),
            pltpu.VMEM(nk.shape, jnp.bfloat16),
            pltpu.VMEM(nv.shape, jnp.bfloat16),
            pltpu.VMEM((8 * sessions, HD), jnp.float32),
            pltpu.VMEM((n_seq, per * 8, HD), jnp.bfloat16),
            pltpu.VMEM((n_seq - 1, per * 8, HD), jnp.bfloat16),
            pltpu.VMEM((n_seq, 8, HD), jnp.float32),
            pltpu.VMEM((n_seq - 1, 8, HD), jnp.float32),
            pltpu.VMEM((n_seq, per * 8, HD), jnp.bfloat16),
            pltpu.VMEM((8 * sessions, HD), jnp.float32),
            dma((8,)),
            dma((2 * n_sends,)),
            dma((2, n_seq * cores)),
            dma((2, n_seq - 1)),
            dma((2, n_seq - 1)),
            dma((n_seq - 1,)),
            dma((n_seq,)),
            pltpu.SemaphoreType.REGULAR((outer,)),
        ],
        compiler_params=pltpu.CompilerParams(
            collective_id=0, has_side_effects=True, vmem_limit_bytes=48 * 1024 * 1024
        ),
    )(
        *(
            x if x.dtype == jnp.int32 else pltpu.with_memory_space_constraint(x, pltpu.HBM)
            for x in args
        )
    )
    return pl.pallas_call(
        store_kernel,
        name="store",
        out_shape=tuple(jax.ShapeDtypeStruct(x.shape, x.dtype) for x in results),
        in_specs=[pl.BlockSpec(memory_space=pl.ANY)] * 2,
        out_specs=(pl.BlockSpec(memory_space=pl.ANY),) * 2,
        scratch_shapes=[dma((2,))],
        compiler_params=pltpu.CompilerParams(vmem_limit_bytes=4 * 1024 * 1024),
    )(*results)


def per_device(outer, inner, cores, *args):
    sessions, span = args[5].shape[0], args[0].shape[0]
    if sessions % (outer * inner) or span % 16 or QH // KVH > 8:
        return composed(*args)
    return fused(outer, inner, cores, *args)


def solution(mesh):
    n_seq, cores = mesh.shape["seq"], mesh.shape["head"]
    inner = max(d for d in range(1, math.isqrt(n_seq) + 1) if n_seq % d == 0)
    return jax.shard_map(
        functools.partial(per_device, n_seq // inner, inner, cores),
        mesh=mesh,
        in_specs=(
            P(("rep", "seq", "head"), None),
            P(("rep", "seq", "head"), None),
            P(("rep", "seq", "head"), None),
            P("rep"),
            P("rep"),
            P("rep", "head"),
            P("rep", "head"),
            P("rep", "head"),
            P("rep", "head", "seq", None),
            P("rep", "head", "seq", None),
            P("rep"),
        ),
        out_specs=(P(("rep", "seq", "head"), None), P("rep", "head")),
        check_vma=False,
    )
```
